256 devices in a mesh: fsdp: 64 (over x, y, z_hi), tp: 4 (over z_lo, core).
Axes of the slice: x: 4, y: 4, z: 8 (z_hi: 4, z_lo: 2; z = z_hi * 2 + z_lo), core: 2. Of those that a mesh axis runs over, the one named last changes fastest.
Arguments:
- momentum: float32 [14336, 4096], P('fsdp', 'tp'), may hold values from -6 to 6
- grad_acc: float32 [14336, 4096], P('fsdp', 'tp'), may hold values from -6 to 6
- query_basis: float32 [4096, 512], P('tp'), may hold values from -6 to 6
- hidden_t: bfloat16 [14336, 8192], P(None, 'fsdp'), may hold values from -6 to 6
- out_grad: bfloat16 [8192, 4096], P('fsdp', 'tp'), may hold values from -0.0625 to 0.0625
Outputs:
- update: float32 [14336, 4096], P('fsdp', 'tp')
- momentum_next: float32 [14336, 4096], P('fsdp', 'tp')
- query_next: float32 [4096, 512], P('tp')
The draws below stay inside these ranges and needn't reach their ends.
All inputs are finite; a program needn't handle non-finite values.
Results may differ from the reference program's by a relative error of at most 0.0003.
Values may be sent and summed in bfloat16 or wider, within the bound.
No kernel may reach another device: no remote copies, remote signals or barrier semaphores. Data moves between devices by JAX's collectives and lax.ppermute only.
A program may use at most 128 MiB of HBM per device.

```python
import math
import jax
import jax.numpy as jnp
from jax import lax

D = 4096
FF = 14336
RANK = 512
TOKENS = 8192


def block_scale(own_key, shape, pieces, low, high):
    def one(dim, blocks):
        steps = jax.random.uniform(jax.random.fold_in(jax.random.fold_in(own_key, 6), dim), (blocks,), jnp.float32, low / len(pieces), high / len(pieces))
        return jnp.repeat(jnp.exp(steps), shape[dim] // blocks).reshape((-1,) + (1,) * (len(shape) - dim - 1))

    level = one(*pieces[0])
    for cut in pieces[1:]:
        level = level * one(*cut)
    return level


def scatter_about(stream_key, shape, scale, most, pieces=(), dtype=jnp.bfloat16):
    drawn = jax.random.normal(stream_key, shape, jnp.float32) * scale
    if len(pieces) > 0:
        drawn = block_scale(stream_key, shape, pieces, -0.22, 0.18) * drawn
    return jnp.clip(drawn, min=-most, max=most).astype(dtype)


def setup_inputs(seed: int = 0) -> dict:
    splits = jax.random.split(jax.random.key(seed), 6)
    return {
        "momentum": scatter_about(splits[0], (FF, D), 1.0, 6.0, ((0, 64), (1, 4)), jnp.float32),
        "grad_acc": scatter_about(splits[1], (FF, D), 1.0, 6.0, ((0, 64), (1, 4)), jnp.float32),
        "query_basis": scatter_about(splits[2], (D, RANK), 1.0, 6.0, ((0, 4),), jnp.float32),
        "hidden_t": scatter_about(splits[3], (FF, TOKENS), 1.0, 6.0, ((1, 64),)),
        "out_grad": scatter_about(splits[4], (TOKENS, D), TOKENS ** -0.5, 0.0625, ((0, 64), (1, 4))),
    }


momentum_keep = 0.95
epsilon = 1e-06

def reference(momentum, grad_acc, query_basis, hidden_t, out_grad):
    highest = lax.Precision.HIGHEST
    micro_grad = jnp.dot(hidden_t.astype(jnp.float32), out_grad.astype(jnp.float32), preferred_element_type=jnp.float32)
    buffer = momentum + grad_acc + micro_grad
    proj = jnp.dot(buffer.astype(jnp.float32), query_basis.astype(jnp.float32), precision=highest, preferred_element_type=jnp.float32)
    gram_sum = jnp.dot(proj.T.astype(jnp.float32), proj.astype(jnp.float32), precision=highest, preferred_element_type=jnp.float32)
    chol_low = jnp.linalg.cholesky(gram_sum)
    ortho = lax.linalg.triangular_solve(chol_low, proj, left_side=False, lower=True, transpose_a=True)
    right_factor = jnp.dot(buffer.T.astype(jnp.float32), ortho.astype(jnp.float32), precision=highest, preferred_element_type=jnp.float32)
    squares = lax.optimization_barrier(jnp.sum(right_factor * right_factor, axis=0))
    query_next = right_factor * lax.rsqrt(squares / D + epsilon)
    momentum_next = buffer - (1.0 - momentum_keep) * jnp.dot(ortho.astype(jnp.float32), right_factor.T.astype(jnp.float32), precision=highest, preferred_element_type=jnp.float32)
    update = math.sqrt(FF / RANK) * jnp.dot(ortho.astype(jnp.float32), query_next.T.astype(jnp.float32), precision=highest, preferred_element_type=jnp.float32)
    return (update, momentum_next, query_next)
```

```python
import math

import jax
import jax.numpy as jnp
from jax import lax
from jax.experimental import pallas as pl
from jax.experimental.pallas import tpu as pltpu
from jax.sharding import Mesh
from jax.sharding import PartitionSpec as P

D = 4096
FF = 14336
RANK = 512
TILE = 128
SUB = 8
CHUNKS = 2

momentum_keep = 0.95
epsilon = 1e-06

ROWS = ("x", "y", "zh")
COLS = ("zl", "core")


def dot(left, right, left_dim, right_dim):
    return lax.dot_general(
        left,
        right,
        (((left_dim,), (right_dim,)), ((), ())),
        precision=lax.Precision.HIGHEST,
        preferred_element_type=jnp.float32,
    )


def eliminate(tile):
    lane = lax.broadcasted_iota(jnp.int32, (SUB, TILE), 1)
    sub = lax.broadcasted_iota(jnp.int32, (SUB, TILE), 0)
    x = [tile[SUB * i : SUB * i + SUB, :] for i in range(TILE // SUB)]
    for p in range(TILE // SUB):
        first = SUB * p
        below = range(p, TILE // SUB)
        cols = [
            {i: jnp.broadcast_to(x[i][:, first + k : first + k + 1], (SUB, TILE)) for i in below}
            for k in range(SUB)
        ]
        inside = (lane >= first) & (lane < first + SUB)
        for i in below:
            eye = (lane == sub + first).astype(jnp.float32) if i == p else 0.0
            x[i] = jnp.where(inside, eye, x[i])
        root = jnp.ones((SUB, TILE), jnp.float32)
        for k in range(SUB):
            pivot = jnp.broadcast_to(cols[k][p][k : k + 1, :], (SUB, TILE))
            inverse = 1.0 / pivot
            root = jnp.where(sub == k, lax.rsqrt(pivot), root)
            mult = {i: cols[k][i] * inverse for i in below}
            mult[p] = jnp.where(sub > k, mult[p], 0.0)
            for m in range(k + 1, SUB):
                head = jnp.broadcast_to(cols[m][p][k : k + 1, :], (SUB, TILE))
                for i in below:
                    cols[m][i] = cols[m][i] - mult[i] * head
            row = jnp.broadcast_to(x[p][k : k + 1, :], (SUB, TILE))
            for i in below:
                x[i] = x[i] - mult[i] * row
        x[p] = jnp.where(lane <= sub + first, x[p] * root, 0.0)
    return jnp.concatenate(x, axis=0)


def inverse_factor_kernel(gram_ref, out_ref, work, small):
    work[...] = gram_ref[...]
    out_ref[...] = jnp.zeros_like(out_ref)

    def step(b, carry):
        corner = pl.multiple_of(b * TILE, TILE)
        small[...] = eliminate(work[pl.ds(corner, TILE), pl.ds(corner, TILE)])
        for s in range(RANK // TILE):

            @pl.when(b == s)
            def _():
                at = s * TILE
                end = at + TILE
                inv = small[...]
                out_ref[at:end, at:end] = inv
                if s > 0:
                    done = dot(inv, work[at:end, :at], 1, 0)
                    out_ref[at:end, :at] = done
                if end < RANK:
                    rest = dot(inv, work[at:end, end:], 1, 0)
                    work[end:, end:] -= dot(rest, rest, 0, 0)
                    work[end:, at:end] = -dot(rest, inv, 0, 0)
                    if s > 0:
                        work[end:, :at] -= dot(rest, done, 0, 0)

        return carry

    lax.fori_loop(0, RANK // TILE, step, 0)


def inverse_factor(gram):
    return pl.pallas_call(
        inverse_factor_kernel,
        out_shape=jax.ShapeDtypeStruct((RANK, RANK), jnp.float32),
        in_specs=[pl.BlockSpec(memory_space=pltpu.VMEM)],
        out_specs=pl.BlockSpec(memory_space=pltpu.VMEM),
        scratch_shapes=[
            pltpu.VMEM((RANK, RANK), jnp.float32),
            pltpu.VMEM((TILE, TILE), jnp.float32),
        ],
        cost_estimate=pl.CostEstimate(
            flops=30_000_000_000, bytes_accessed=8 * RANK * RANK, transcendentals=0
        ),
        name="inverse_factor",
    )(gram)


def swap(pieces, axes):
    return lax.all_to_all(pieces, axes, 0, 0, tiled=True)


def to_all(piece, axes):
    devices = lax.axis_size(axes)
    return swap(jnp.broadcast_to(piece[None], (devices, *piece.shape)), axes)


def ring(by, turned=False):
    other = -by if turned else by
    return [(2 * z + c, 2 * ((z + (other if c else by)) % 4) + c) for z in range(4) for c in range(2)]


def neighbours(value, by):
    return lax.ppermute(value, ("zh", "core"), ring(by, turned=True))


def flip(value, axis):
    return lax.ppermute(value, axis, [(0, 1), (1, 0)])


def part(stack, index, dim=0):
    return lax.dynamic_index_in_dim(stack, index, dim, keepdims=False)


def sum_at_owner(stack, axis):
    me = lax.axis_index(axis)
    total = part(stack, me)
    arrived = []
    for by in range(1, 4):
        pairs = [(i, (i + by) % 4) for i in range(4)]
        arrived.append(lax.ppermute(part(stack, (me + by) % 4), axis, pairs))
    return total + arrived[0] + arrived[1] + arrived[2]


def summed_micro_grad(mine, other, grads):
    even = lax.axis_index("core") == 0

    def product(hidden):
        return lax.dot_general(
            hidden,
            grads.reshape(16, -1, grads.shape[1]),
            (((0, 3), (0, 1)), ((), ())),
            preferred_element_type=jnp.float32,
        )

    here, there = product(mine), product(other)
    own = jnp.where(even, here[0], there[0])
    across = jnp.where(even, there[0], here[0])
    ahead, behind = here[1], there[1]
    half = own.shape[0] // 2
    ahead_far = neighbours(across[:half], 1)
    behind_far = neighbours(across[half:], -1)
    from_ahead = neighbours(ahead[half:], 1)
    from_behind = neighbours(behind[:half], -1)
    from_ahead_far = neighbours(ahead[:half] + ahead_far, 1)
    from_behind_far = neighbours(behind[half:] + behind_far, -1)
    return jnp.concatenate(
        [own[:half] + from_behind + from_ahead_far, own[half:] + from_ahead + from_behind_far]
    )


def per_device(momentum, grad_acc, query_basis, hidden_t, out_grad):
    rows, features = momentum.shape
    tokens = hidden_t.shape[1]
    z, core = lax.axis_index("zh"), lax.axis_index("core")
    blocks = hidden_t.reshape(16, 4, rows, tokens)
    wanted = jnp.stack([part(blocks, (z + 2 * core + k) % 4, 1) for k in range(2)], axis=1)
    mine = swap(wanted, ("x", "y"))
    other = flip(mine, "core")
    width = features // CHUNKS
    buffers, partial_proj = [], 0.0
    for k in range(CHUNKS):
        at = slice(k * width, (k + 1) * width)
        grads = lax.all_gather(out_grad[:, at], ("x", "y"), axis=0, tiled=True)
        micro_grad = summed_micro_grad(mine, other, grads)
        buffers.append(momentum[:, at] + grad_acc[:, at] + micro_grad)
        partial_proj = partial_proj + dot(buffers[-1], query_basis[at], 1, 0)
    buffer = jnp.concatenate(buffers, axis=1)

    chip_proj = partial_proj + flip(partial_proj, "core")
    proj = chip_proj + flip(chip_proj, "zl")
    first = lax.axis_index(COLS) * TILE
    strip = dot(lax.dynamic_slice_in_dim(proj, first, TILE, 1), proj, 0, 0)
    tiles = strip.reshape(16, 8, 4, 128).transpose(0, 2, 1, 3).reshape(64, 8, 128)
    tiles = to_all(swap(tiles, ROWS).sum(axis=0), ROWS)
    strip = tiles.reshape(16, 4, 8, 128).transpose(0, 2, 1, 3).reshape(TILE, RANK)
    gram = to_all(strip, COLS).reshape(RANK, RANK)

    mixed = dot(buffer, proj, 0, 0)
    for axis in ROWS:
        mixed = sum_at_owner(mixed.reshape(4, -1, RANK), axis)
    mixed = to_all(mixed, "zh").reshape(-1, RANK)
    mixed = lax.all_gather(mixed, ("x", "y"), axis=0, tiled=True)

    inv = inverse_factor(gram)
    ortho = dot(proj, inv, 1, 1)
    right = dot(mixed, inv, 1, 1)
    squares = to_all(jnp.sum(right * right, axis=0)[None], COLS).sum(axis=(0, 1))
    momentum_next = buffer - (1.0 - momentum_keep) * dot(ortho, right, 1, 1)
    query_next = right * lax.rsqrt(squares / D + epsilon)
    update = math.sqrt(FF / RANK) * dot(ortho, query_next, 1, 1)
    return (update, momentum_next, query_next)


def solution(mesh):
    fine = Mesh(mesh.devices.reshape(4, 4, 4, 2, 2), ROWS + COLS)
    return jax.shard_map(
        per_device,
        mesh=fine,
        in_specs=(
            P(ROWS, COLS),
            P(ROWS, COLS),
            P(COLS, None),
            P(None, ROWS),
            P(ROWS, COLS),
        ),
        out_specs=(P(ROWS, COLS), P(ROWS, COLS), P(COLS, None)),
        check_vma=False,
    )
```

```python
import math

import jax
import jax.numpy as jnp
from jax import lax
from jax.experimental import pallas as pl
from jax.experimental.pallas import tpu as pltpu
from jax.sharding import Mesh
from jax.sharding import PartitionSpec as P


D = 4096
FF = 14336
RANK = 512
TILE = 128
SUB = 8
CHUNKS = 2

momentum_keep = 0.95
epsilon = 1e-06

ROWS = ("x", "y", "zh")
COLS = ("zl", "core")
PLANE = ("x", "y")


def dot(left, right, left_dim, right_dim):
    return lax.dot_general(
        left,
        right,
        (((left_dim,), (right_dim,)), ((), ())),
        precision=lax.Precision.HIGHEST,
        preferred_element_type=jnp.float32,
    )


def eliminate(tile):
    lane = lax.broadcasted_iota(jnp.int32, (SUB, TILE), 1)
    sub = lax.broadcasted_iota(jnp.int32, (SUB, TILE), 0)
    x = [tile[SUB * i : SUB * i + SUB, :] for i in range(TILE // SUB)]
    for p in range(TILE // SUB):
        first = SUB * p
        below = range(p, TILE // SUB)
        cols = [
            {i: jnp.broadcast_to(x[i][:, first + k : first + k + 1], (SUB, TILE)) for i in below}
            for k in range(SUB)
        ]
        inside = (lane >= first) & (lane < first + SUB)
        for i in below:
            eye = (lane == sub + first).astype(jnp.float32) if i == p else 0.0
            x[i] = jnp.where(inside, eye, x[i])
        root = jnp.ones((SUB, TILE), jnp.float32)
        for k in range(SUB):
            pivot = jnp.broadcast_to(cols[k][p][k : k + 1, :], (SUB, TILE))
            inverse = 1.0 / pivot
            root = jnp.where(sub == k, lax.rsqrt(pivot), root)
            mult = {i: cols[k][i] * inverse for i in below}
            mult[p] = jnp.where(sub > k, mult[p], 0.0)
            for m in range(k + 1, SUB):
                head = jnp.broadcast_to(cols[m][p][k : k + 1, :], (SUB, TILE))
                for i in below:
                    cols[m][i] = cols[m][i] - mult[i] * head
            row = jnp.broadcast_to(x[p][k : k + 1, :], (SUB, TILE))
            for i in below:
                x[i] = x[i] - mult[i] * row
        x[p] = jnp.where(lane <= sub + first, x[p] * root, 0.0)
    return jnp.concatenate(x, axis=0)


def inverse_factor_kernel(gram_ref, out_ref, work, small):
    work[...] = gram_ref[...]
    out_ref[...] = jnp.zeros_like(out_ref)

    def step(b, carry):
        corner = pl.multiple_of(b * TILE, TILE)
        small[...] = eliminate(work[pl.ds(corner, TILE), pl.ds(corner, TILE)])
        for s in range(RANK // TILE):

            @pl.when(b == s)
            def _():
                at = s * TILE
                end = at + TILE
                inv = small[...]
                out_ref[at:end, at:end] = inv
                if s > 0:
                    done = dot(inv, work[at:end, :at], 1, 0)
                    out_ref[at:end, :at] = done
                if end < RANK:
                    rest = dot(inv, work[at:end, end:], 1, 0)
                    work[end:, end:] -= dot(rest, rest, 0, 0)
                    work[end:, at:end] = -dot(rest, inv, 0, 0)
                    if s > 0:
                        work[end:, :at] -= dot(rest, done, 0, 0)

        return carry

    lax.fori_loop(0, RANK // TILE, step, 0)


def inverse_factor(gram):
    return pl.pallas_call(
        inverse_factor_kernel,
        out_shape=jax.ShapeDtypeStruct((RANK, RANK), jnp.float32),
        in_specs=[pl.BlockSpec(memory_space=pltpu.VMEM)],
        out_specs=pl.BlockSpec(memory_space=pltpu.VMEM),
        scratch_shapes=[
            pltpu.VMEM((RANK, RANK), jnp.float32),
            pltpu.VMEM((TILE, TILE), jnp.float32),
        ],
        cost_estimate=pl.CostEstimate(
            flops=30_000_000_000, bytes_accessed=8 * RANK * RANK, transcendentals=0
        ),
        name="inverse_factor",
    )(gram)


def swap(pieces, axes):
    return lax.all_to_all(pieces, axes, 0, 0, tiled=True)


def to_all(piece, axes):
    devices = lax.axis_size(axes)
    return swap(jnp.broadcast_to(piece[None], (devices, *piece.shape)), axes)


def ring(by, turned=False):
    other = -by if turned else by
    return [(2 * z + c, 2 * ((z + (other if c else by)) % 4) + c) for z in range(4) for c in range(2)]


def neighbours(value, by):
    return lax.ppermute(value, ("zh", "core"), ring(by, turned=True))


def flip(value, axis):
    return lax.ppermute(value, axis, [(0, 1), (1, 0)])


def part(stack, index, dim=0):
    return lax.dynamic_index_in_dim(stack, index, dim, keepdims=False)


def sum_at_owner(rows, axes):
    devices = lax.axis_size(axes)
    return swap(rows.reshape(devices, -1, rows.shape[-1]), axes).sum(axis=0)


def from_owners(rows, axes):
    return to_all(rows, axes).reshape(-1, rows.shape[-1])


def turns(value, axis, by):
    return lax.ppermute(value, axis, [(i, (i + by) % 4) for i in range(4)])


def sum_round(rows, axis):
    me = lax.axis_index(axis)
    pieces = rows.reshape(4, -1, rows.shape[-1])
    arrived = [turns(part(pieces, (me + by) % 4), axis, by) for by in range(1, 4)]
    return part(pieces, me) + arrived[0] + arrived[1] + arrived[2]


def collect_round(piece, axis):
    me = lax.axis_index(axis)
    whole = jnp.zeros((4, *piece.shape), piece.dtype)
    for by in range(4):
        came = turns(piece, axis, by) if by else piece
        whole = lax.dynamic_update_index_in_dim(whole, came, (me - by) % 4, 0)
    return whole.reshape(-1, piece.shape[-1])


def summed_micro_grad(mine, other, grads):
    even = lax.axis_index("core") == 0

    def product(hidden):
        return lax.dot_general(
            hidden, grads, (((0, 3), (0, 1)), ((), ())), preferred_element_type=jnp.float32
        )

    here = product(mine)
    there = product(other)
    own = jnp.where(even, here[0], there[0])
    across = jnp.where(even, there[0], here[0])
    half = own.shape[0] // 2
    ahead_far = neighbours(across[:half], 1)
    behind_far = neighbours(across[half:], -1)
    ahead = jnp.concatenate([here[1][:half] + ahead_far, here[1][half:]])
    behind = jnp.concatenate([there[1][:half], there[1][half:] + behind_far])
    ahead = neighbours(ahead, 1)
    behind = neighbours(behind, -1)
    return own + ahead + behind


def per_device(momentum, grad_acc, query_basis, hidden_t, out_grad):
    rows, features = momentum.shape
    tokens = hidden_t.shape[1]
    z, core = lax.axis_index("zh"), lax.axis_index("core")
    blocks = hidden_t.reshape(16, 4, rows, tokens)
    wanted = jnp.stack([part(blocks, (z + 2 * core + k) % 4, 1) for k in range(2)], axis=1)
    mine = swap(wanted, PLANE)
    width = features // CHUNKS
    grads = []
    for k in range(CHUNKS):
        grads.append(to_all(out_grad[:, k * width : (k + 1) * width], PLANE))
    other = flip(mine, "core")
    buffers, partial_proj = [], 0.0
    for k in range(CHUNKS):
        at = slice(k * width, (k + 1) * width)
        micro_grad = summed_micro_grad(mine, other, grads[k])
        buffers.append(momentum[:, at] + grad_acc[:, at] + micro_grad)
        partial_proj = partial_proj + dot(buffers[-1], query_basis[at], 1, 0)
    buffer = jnp.concatenate(buffers, axis=1)

    chip_proj = partial_proj + flip(partial_proj, "core")
    proj = chip_proj + flip(chip_proj, "zl")
    first = lax.axis_index(COLS) * TILE
    strip = dot(lax.dynamic_slice_in_dim(proj, first, TILE, 1), proj, 0, 0)
    strip, proj = lax.optimization_barrier((strip, proj))
    mixed = dot(buffer, proj, 0, 0)

    strip = sum_at_owner(strip, PLANE)
    mixed = sum_round(mixed, "x")
    strip = sum_at_owner(strip, "zh")
    strip = from_owners(strip, "zh")
    strip = from_owners(strip, PLANE)
    mixed = sum_round(mixed, "y")
    gram = from_owners(strip, COLS)
    mixed = sum_round(mixed, "zh")
    mixed = collect_round(mixed, "zh")
    gram, mixed = lax.optimization_barrier((gram, mixed))
    mixed = from_owners(mixed, PLANE)

    inv = inverse_factor(gram)
    ortho = dot(proj, inv, 1, 1)
    right = dot(mixed, inv, 1, 1)
    squares = to_all(jnp.sum(right * right, axis=0)[None], COLS).sum(axis=(0, 1))
    momentum_next = buffer - (1.0 - momentum_keep) * dot(ortho, right, 1, 1)
    query_next = right * lax.rsqrt(squares / D + epsilon)
    update = math.sqrt(FF / RANK) * dot(ortho, query_next, 1, 1)
    return (update, momentum_next, query_next)


def solution(mesh):
    fine = Mesh(mesh.devices.reshape(4, 4, 4, 2, 2), ROWS + COLS)
    return jax.shard_map(
        per_device,
        mesh=fine,
        in_specs=(
            P(ROWS, COLS),
            P(ROWS, COLS),
            P(COLS, None),
            P(None, ROWS),
            P(ROWS, COLS),
        ),
        out_specs=(P(ROWS, COLS), P(ROWS, COLS), P(COLS, None)),
        check_vma=False,
    )
```

```python
import math

import jax
import jax.numpy as jnp
from jax import lax
from jax.experimental import pallas as pl
from jax.experimental.pallas import tpu as pltpu
from jax.sharding import Mesh
from jax.sharding import PartitionSpec as P


D = 4096
FF = 14336
RANK = 512
TILE = 128
SUB = 8
CHUNKS = 2

momentum_keep = 0.95
epsilon = 1e-06

ROWS = ("x", "y", "zh")
COLS = ("zl", "core")
PLANE = ("x", "y")
FEWER = lax.Precision.HIGH


def dot(left, right, left_dim, right_dim, precision=lax.Precision.HIGHEST):
    return lax.dot_general(
        left,
        right,
        (((left_dim,), (right_dim,)), ((), ())),
        precision=precision,
        preferred_element_type=jnp.float32,
    )


def eliminate(tile):
    lane = lax.broadcasted_iota(jnp.int32, (SUB, TILE), 1)
    sub = lax.broadcasted_iota(jnp.int32, (SUB, TILE), 0)
    x = [tile[SUB * i : SUB * i + SUB, :] for i in range(TILE // SUB)]
    for p in range(TILE // SUB):
        first = SUB * p
        below = range(p, TILE // SUB)
        cols = [
            {i: jnp.broadcast_to(x[i][:, first + k : first + k + 1], (SUB, TILE)) for i in below}
            for k in range(SUB)
        ]
        inside = (lane >= first) & (lane < first + SUB)
        for i in below:
            eye = (lane == sub + first).astype(jnp.float32) if i == p else 0.0
            x[i] = jnp.where(inside, eye, x[i])
        root = jnp.ones((SUB, TILE), jnp.float32)
        for k in range(SUB):
            pivot = jnp.broadcast_to(cols[k][p][k : k + 1, :], (SUB, TILE))
            inverse = 1.0 / pivot
            root = jnp.where(sub == k, lax.rsqrt(pivot), root)
            mult = {i: cols[k][i] * inverse for i in below}
            mult[p] = jnp.where(sub > k, mult[p], 0.0)
            for m in range(k + 1, SUB):
                head = jnp.broadcast_to(cols[m][p][k : k + 1, :], (SUB, TILE))
                for i in below:
                    cols[m][i] = cols[m][i] - mult[i] * head
            row = jnp.broadcast_to(x[p][k : k + 1, :], (SUB, TILE))
            for i in below:
                x[i] = x[i] - mult[i] * row
        x[p] = jnp.where(lane <= sub + first, x[p] * root, 0.0)
    return jnp.concatenate(x, axis=0)


def inverse_factor_kernel(gram_ref, out_ref, work, small):
    for tile in range(16):
        for column in range(4):
            row = column * TILE + tile * SUB
            work[row : row + SUB, :] = gram_ref[tile, column]
    out_ref[...] = jnp.zeros_like(out_ref)

    def step(b, carry):
        corner = pl.multiple_of(b * TILE, TILE)
        small[...] = eliminate(work[pl.ds(corner, TILE), pl.ds(corner, TILE)])
        for s in range(RANK // TILE):

            @pl.when(b == s)
            def _():
                at = s * TILE
                end = at + TILE
                inv = small[...]
                out_ref[at:end, at:end] = inv
                if s > 0:
                    done = dot(inv, work[at:end, :at], 1, 0)
                    out_ref[at:end, :at] = done
                if end < RANK:
                    rest = dot(inv, work[at:end, end:], 1, 0)
                    work[end:, end:] -= dot(rest, rest, 0, 0)
                    work[end:, at:end] = -dot(rest, inv, 0, 0)
                    if s > 0:
                        work[end:, :at] -= dot(rest, done, 0, 0)

        return carry

    lax.fori_loop(0, RANK // TILE, step, 0)


def inverse_factor(gram):
    return pl.pallas_call(
        inverse_factor_kernel,
        out_shape=jax.ShapeDtypeStruct((RANK, RANK), jnp.float32),
        in_specs=[pl.BlockSpec(memory_space=pltpu.VMEM)],
        out_specs=pl.BlockSpec(memory_space=pltpu.VMEM),
        scratch_shapes=[
            pltpu.VMEM((RANK, RANK), jnp.float32),
            pltpu.VMEM((TILE, TILE), jnp.float32),
        ],
        cost_estimate=pl.CostEstimate(
            flops=30_000_000_000, bytes_accessed=8 * RANK * RANK, transcendentals=0
        ),
        name="inverse_factor",
    )(gram)


def swap(pieces, axes):
    return lax.all_to_all(pieces, axes, 0, 0, tiled=True)


def to_all(piece, axes):
    devices = lax.axis_size(axes)
    return swap(jnp.broadcast_to(piece[None], (devices, *piece.shape)), axes)


def ring(by, turned=False):
    other = -by if turned else by
    return [(2 * z + c, 2 * ((z + (other if c else by)) % 4) + c) for z in range(4) for c in range(2)]


def neighbours(value, by):
    return lax.ppermute(value, ("zh", "core"), ring(by, turned=True))


def flip(value, axis):
    return lax.ppermute(value, axis, [(0, 1), (1, 0)])


def part(stack, index, dim=0):
    return lax.dynamic_index_in_dim(stack, index, dim, keepdims=False)


def from_owners(rows, axes):
    return to_all(rows, axes).reshape(-1, rows.shape[-1])


def turns(value, axis, by):
    return lax.ppermute(value, axis, [(i, (i + by) % 4) for i in range(4)])


def collect_round(piece, axis):
    me = lax.axis_index(axis)
    whole = jnp.zeros((4, *piece.shape), piece.dtype)
    for by in range(4):
        came = turns(piece, axis, by) if by else piece
        whole = lax.dynamic_update_index_in_dim(whole, came, (me - by) % 4, 0)
    return whole.reshape(-1, piece.shape[-1])


def ring_total(value, axis):
    came = [turns(value, axis, by) for by in range(1, 4)]
    return (value + came[1]) + (came[0] + came[2])


def summed_micro_grad(mine, other, grads):
    even = lax.axis_index("core") == 0

    def product(hidden):
        return lax.dot_general(
            hidden, grads, (((0, 3), (0, 1)), ((), ())), preferred_element_type=jnp.float32
        )

    here = product(mine)
    there = product(other)
    own = jnp.where(even, here[0], there[0])
    across = jnp.where(even, there[0], here[0])

    def code(block):
        top = jnp.maximum(jnp.max(jnp.abs(block), axis=0, keepdims=True), 1e-30)
        power = jnp.ceil(jnp.log2(top)) - 14.0
        coded = (block * jnp.exp2(-power)).astype(jnp.float16)
        return jnp.concatenate([coded, jnp.broadcast_to(power, (16, block.shape[1])).astype(jnp.float16)])

    def sent(coded, by):
        came = neighbours(coded, by).astype(jnp.float32)
        return came[:-16] * jnp.exp2(came[-1:])

    coded = [code(here[1]), code(across), code(there[1])]
    total = own + (sent(coded[0], 1) + sent(coded[1], 2) + sent(coded[2], -1))
    mine, other, *_ = lax.optimization_barrier((mine, other, *coded))
    return total, mine, other


def per_device(momentum, grad_acc, query_basis, hidden_t, out_grad):
    rows, features = momentum.shape
    tokens = hidden_t.shape[1]
    z, core = lax.axis_index("zh"), lax.axis_index("core")
    blocks = hidden_t.reshape(16, 4, rows, tokens)
    wanted = jnp.stack([part(blocks, (z + 2 * core + k) % 4, 1) for k in range(2)], axis=1)
    mine = swap(wanted, PLANE)
    width = features // CHUNKS
    grads = []
    for k in range(CHUNKS):
        grads.append(to_all(out_grad[:, k * width : (k + 1) * width], PLANE))
    other = flip(mine, "core")
    buffers, partial_proj = [], 0.0
    for k in range(CHUNKS):
        at = slice(k * width, (k + 1) * width)
        micro_grad, mine, other = summed_micro_grad(mine, other, grads[k])
        buffers.append(momentum[:, at] + grad_acc[:, at] + micro_grad)
        partial_proj = partial_proj + dot(buffers[-1], query_basis[at], 1, 0)
    buffer = jnp.concatenate(buffers, axis=1)

    chip_proj = partial_proj + flip(partial_proj, "core")
    proj = chip_proj + flip(chip_proj, "zl")
    first = lax.axis_index(COLS) * TILE
    strip = dot(lax.dynamic_slice_in_dim(proj, first, TILE, 1), proj, 0, 0)
    strip, proj = lax.optimization_barrier((strip, proj))
    mixed = dot(buffer, proj, 0, 0)

    both = jnp.concatenate([mixed.reshape(16, -1, RANK), strip.reshape(16, -1, RANK)], axis=1)
    both = swap(both, PLANE).sum(axis=0)
    mixed, strip = both[:-SUB], both[-SUB:]
    strip = to_all(strip, "zh").sum(axis=0)
    mixed = ring_total(mixed, "zh")
    strip = from_owners(strip, COLS)
    gram = to_all(strip, PLANE).reshape(16, 4, SUB, RANK)
    mixed = collect_round(mixed, "y")
    gram, mixed = lax.optimization_barrier((gram, mixed))
    mixed = from_owners(mixed, "x")

    inv = inverse_factor(gram)
    ortho = dot(proj, inv, 1, 1, FEWER)
    right = dot(mixed, inv, 1, 1, FEWER)
    squares = to_all(jnp.sum(right * right, axis=0)[None], COLS).sum(axis=(0, 1))
    momentum_next = buffer - (1.0 - momentum_keep) * dot(ortho, right, 1, 1, FEWER)
    query_next = right * lax.rsqrt(squares / D + epsilon)
    update = math.sqrt(FF / RANK) * dot(ortho, query_next, 1, 1, FEWER)
    return (update, momentum_next, query_next)


def solution(mesh):
    fine = Mesh(mesh.devices.reshape(4, 4, 4, 2, 2), ROWS + COLS)
    return jax.shard_map(
        per_device,
        mesh=fine,
        in_specs=(
            P(ROWS, COLS),
            P(ROWS, COLS),
            P(COLS, None),
            P(None, ROWS),
            P(ROWS, COLS),
        ),
        out_specs=(P(ROWS, COLS), P(ROWS, COLS), P(COLS, None)),
        check_vma=False,
    )
```

```python
import math

import jax
import jax.numpy as jnp
from jax import lax
from jax.experimental import pallas as pl
from jax.experimental.pallas import tpu as pltpu
from jax.sharding import Mesh
from jax.sharding import PartitionSpec as P


D = 4096
FF = 14336
RANK = 512
TILE = 128
SUB = 8
CHUNKS = 2

momentum_keep = 0.95
epsilon = 1e-06

ROWS = ("x", "y", "zh")
COLS = ("zl", "core")
PLANE = ("x", "y")
FEWER = lax.Precision.HIGH


def dot(left, right, left_dim, right_dim, precision=lax.Precision.HIGHEST):
    return lax.dot_general(
        left,
        right,
        (((left_dim,), (right_dim,)), ((), ())),
        precision=precision,
        preferred_element_type=jnp.float32,
    )


def eliminate(tile):
    lane = lax.broadcasted_iota(jnp.int32, (SUB, TILE), 1)
    sub = lax.broadcasted_iota(jnp.int32, (SUB, TILE), 0)
    x = [tile[SUB * i : SUB * i + SUB, :] for i in range(TILE // SUB)]
    for p in range(TILE // SUB):
        first = SUB * p
        below = range(p, TILE // SUB)
        cols = [
            {i: jnp.broadcast_to(x[i][:, first + k : first + k + 1], (SUB, TILE)) for i in below}
            for k in range(SUB)
        ]
        inside = (lane >= first) & (lane < first + SUB)
        for i in below:
            eye = (lane == sub + first).astype(jnp.float32) if i == p else 0.0
            x[i] = jnp.where(inside, eye, x[i])
        root = jnp.ones((SUB, TILE), jnp.float32)
        for k in range(SUB):
            pivot = jnp.broadcast_to(cols[k][p][k : k + 1, :], (SUB, TILE))
            inverse = 1.0 / pivot
            root = jnp.where(sub == k, lax.rsqrt(pivot), root)
            mult = {i: cols[k][i] * inverse for i in below}
            mult[p] = jnp.where(sub > k, mult[p], 0.0)
            for m in range(k + 1, SUB):
                head = jnp.broadcast_to(cols[m][p][k : k + 1, :], (SUB, TILE))
                for i in below:
                    cols[m][i] = cols[m][i] - mult[i] * head
            row = jnp.broadcast_to(x[p][k : k + 1, :], (SUB, TILE))
            for i in below:
                x[i] = x[i] - mult[i] * row
        x[p] = jnp.where(lane <= sub + first, x[p] * root, 0.0)
    return jnp.concatenate(x, axis=0)


def inverse_factor_kernel(gram_ref, out_ref, work, small):
    for tile in range(16):
        for column in range(4):
            row = column * TILE + tile * SUB
            work[row : row + SUB, :] = gram_ref[tile, column]
    out_ref[...] = jnp.zeros_like(out_ref)

    def step(b, carry):
        corner = pl.multiple_of(b * TILE, TILE)
        small[...] = eliminate(work[pl.ds(corner, TILE), pl.ds(corner, TILE)])
        for s in range(RANK // TILE):

            @pl.when(b == s)
            def _():
                at = s * TILE
                end = at + TILE
                inv = small[...]
                out_ref[at:end, at:end] = inv
                if s > 0:
                    done = dot(inv, work[at:end, :at], 1, 0)
                    out_ref[at:end, :at] = done
                if end < RANK:
                    rest = dot(inv, work[at:end, end:], 1, 0)
                    work[end:, end:] -= dot(rest, rest, 0, 0)
                    work[end:, at:end] = -dot(rest, inv, 0, 0)
                    if s > 0:
                        work[end:, :at] -= dot(rest, done, 0, 0)

        return carry

    lax.fori_loop(0, RANK // TILE, step, 0)


def inverse_factor(gram):
    return pl.pallas_call(
        inverse_factor_kernel,
        out_shape=jax.ShapeDtypeStruct((RANK, RANK), jnp.float32),
        in_specs=[pl.BlockSpec(memory_space=pltpu.VMEM)],
        out_specs=pl.BlockSpec(memory_space=pltpu.VMEM),
        scratch_shapes=[
            pltpu.VMEM((RANK, RANK), jnp.float32),
            pltpu.VMEM((TILE, TILE), jnp.float32),
        ],
        cost_estimate=pl.CostEstimate(
            flops=30_000_000_000, bytes_accessed=8 * RANK * RANK, transcendentals=0
        ),
        name="inverse_factor",
    )(gram)


def swap(pieces, axes):
    return lax.all_to_all(pieces, axes, 0, 0, tiled=True)


def to_all(piece, axes):
    devices = lax.axis_size(axes)
    return swap(jnp.broadcast_to(piece[None], (devices, *piece.shape)), axes)


def ring(by, turned=False):
    other = -by if turned else by
    return [(2 * z + c, 2 * ((z + (other if c else by)) % 4) + c) for z in range(4) for c in range(2)]


def neighbours(value, by):
    return lax.ppermute(value, ("zh", "core"), ring(by, turned=True))


def flip(value, axis):
    return lax.ppermute(value, axis, [(0, 1), (1, 0)])


def part(stack, index, dim=0):
    return lax.dynamic_index_in_dim(stack, index, dim, keepdims=False)


def from_owners(rows, axes):
    return to_all(rows, axes).reshape(-1, rows.shape[-1])


def turns(value, axis, by):
    return lax.ppermute(value, axis, [(i, (i + by) % 4) for i in range(4)])


def collect_round(piece, axis, dim=0):
    me = lax.axis_index(axis)
    came = [turns(piece, axis, by) for by in range(1, 4)]
    whole = jnp.stack([piece] * 4, axis=dim)
    for by in range(1, 4):
        whole = lax.dynamic_update_index_in_dim(whole, came[by - 1], (me - by) % 4, dim)
    return whole


def ring_total(value, axis):
    came = [turns(value, axis, by) for by in range(1, 4)]
    return (value + came[1]) + (came[0] + came[2])


def summed_micro_grad(mine, other, grads):
    even = lax.axis_index("core") == 0

    def product(hidden):
        return lax.dot_general(
            hidden, grads, (((0, 3), (0, 1)), ((), ())), preferred_element_type=jnp.float32
        )

    here = product(mine)
    there = product(other)
    own = jnp.where(even, here[0], there[0])
    across = jnp.where(even, there[0], here[0])

    def code(block):
        top = jnp.maximum(jnp.max(jnp.abs(block), axis=0, keepdims=True), 1e-30)
        power = jnp.ceil(jnp.log2(top)) - 14.0
        coded = (block * jnp.exp2(-power)).astype(jnp.float16)
        return jnp.concatenate([coded, jnp.broadcast_to(power, (16, block.shape[1])).astype(jnp.float16)])

    def sent(coded, by):
        came = neighbours(coded, by).astype(jnp.float32)
        return came[:-16] * jnp.exp2(came[-1:])

    coded = [code(here[1]), code(across), code(there[1])]
    total = own + (sent(coded[0], 1) + sent(coded[1], 2) + sent(coded[2], -1))
    mine, other, *_ = lax.optimization_barrier((mine, other, *coded))
    return total, mine, other


def per_device(momentum, grad_acc, query_basis, hidden_t, out_grad):
    rows, features = momentum.shape
    tokens = hidden_t.shape[1]
    z, core = lax.axis_index("zh"), lax.axis_index("core")
    blocks = hidden_t.reshape(16, 4, rows, tokens)
    wanted = jnp.stack([part(blocks, (z + 2 * core + k) % 4, 1) for k in range(2)], axis=1)
    mine = swap(wanted, PLANE)
    width = features // CHUNKS
    grads = []
    for k in range(CHUNKS):
        piece = out_grad[:, k * width : (k + 1) * width]
        piece = collect_round(piece, PLANE[k])
        piece = collect_round(piece, PLANE[1 - k], 1 - k)
        grads.append(piece.reshape(16, tokens, width))
    other = flip(mine, "core")
    buffers, partial_proj = [], 0.0
    for k in range(CHUNKS):
        at = slice(k * width, (k + 1) * width)
        micro_grad, mine, other = summed_micro_grad(mine, other, grads[k])
        buffers.append(momentum[:, at] + grad_acc[:, at] + micro_grad)
        partial_proj = partial_proj + dot(buffers[-1], query_basis[at], 1, 0)
    buffer = jnp.concatenate(buffers, axis=1)

    chip_proj = partial_proj + flip(partial_proj, "core")
    proj = chip_proj + flip(chip_proj, "zl")
    first = lax.axis_index(COLS) * TILE
    strip = dot(lax.dynamic_slice_in_dim(proj, first, TILE, 1), proj, 0, 0)
    strip, proj = lax.optimization_barrier((strip, proj))
    mixed = dot(buffer, proj, 0, 0)

    both = jnp.concatenate([mixed.reshape(16, -1, RANK), strip.reshape(16, -1, RANK)], axis=1)
    both = swap(both, PLANE).sum(axis=0)
    mixed, strip = both[:-SUB], both[-SUB:]
    strip = to_all(strip, "zh").sum(axis=0)
    mixed = ring_total(mixed, "zh")
    strip = from_owners(strip, COLS)
    gram = to_all(strip, PLANE).reshape(16, 4, SUB, RANK)
    mixed = collect_round(mixed, "y").reshape(-1, RANK)
    mixed = collect_round(mixed, "x").reshape(-1, RANK)

    inv = inverse_factor(gram)
    ortho = dot(proj, inv, 1, 1, FEWER)
    right = dot(mixed, inv, 1, 1, FEWER)
    squares = to_all(jnp.sum(right * right, axis=0)[None], COLS).sum(axis=(0, 1))
    momentum_next = buffer - (1.0 - momentum_keep) * dot(ortho, right, 1, 1, FEWER)
    query_next = right * lax.rsqrt(squares / D + epsilon)
    update = math.sqrt(FF / RANK) * dot(ortho, query_next, 1, 1, FEWER)
    return (update, momentum_next, query_next)


def solution(mesh):
    fine = Mesh(mesh.devices.reshape(4, 4, 4, 2, 2), ROWS + COLS)
    return jax.shard_map(
        per_device,
        mesh=fine,
        in_specs=(
            P(ROWS, COLS),
            P(ROWS, COLS),
            P(COLS, None),
            P(None, ROWS),
            P(ROWS, COLS),
        ),
        out_specs=(P(ROWS, COLS), P(ROWS, COLS), P(COLS, None)),
        check_vma=False,
    )
```

```python
import math

import jax
import jax.numpy as jnp
from jax import lax
from jax.experimental import pallas as pl
from jax.experimental.pallas import tpu as pltpu
from jax.sharding import Mesh
from jax.sharding import PartitionSpec as P


D = 4096
FF = 14336
RANK = 512
TILE = 128
SUB = 8
CHUNKS = 2

momentum_keep = 0.95
epsilon = 1e-06

ROWS = ("x", "y", "zh")
COLS = ("zl", "core")
PLANE = ("x", "y")
FEWER = lax.Precision.HIGH


def dot(left, right, left_dim, right_dim, precision=lax.Precision.HIGHEST):
    return lax.dot_general(
        left,
        right,
        (((left_dim,), (right_dim,)), ((), ())),
        precision=precision,
        preferred_element_type=jnp.float32,
    )


def eliminate(tile):
    lane = lax.broadcasted_iota(jnp.int32, (SUB, TILE), 1)
    sub = lax.broadcasted_iota(jnp.int32, (SUB, TILE), 0)
    x = [tile[SUB * i : SUB * i + SUB, :] for i in range(TILE // SUB)]
    for p in range(TILE // SUB):
        first = SUB * p
        below = range(p, TILE // SUB)
        cols = [
            {i: jnp.broadcast_to(x[i][:, first + k : first + k + 1], (SUB, TILE)) for i in below}
            for k in range(SUB)
        ]
        inside = (lane >= first) & (lane < first + SUB)
        for i in below:
            eye = (lane == sub + first).astype(jnp.float32) if i == p else 0.0
            x[i] = jnp.where(inside, eye, x[i])
        root = jnp.ones((SUB, TILE), jnp.float32)
        for k in range(SUB):
            pivot = jnp.broadcast_to(cols[k][p][k : k + 1, :], (SUB, TILE))
            inverse = 1.0 / pivot
            root = jnp.where(sub == k, lax.rsqrt(pivot), root)
            mult = {i: cols[k][i] * inverse for i in below}
            mult[p] = jnp.where(sub > k, mult[p], 0.0)
            for m in range(k + 1, SUB):
                head = jnp.broadcast_to(cols[m][p][k : k + 1, :], (SUB, TILE))
                for i in below:
                    cols[m][i] = cols[m][i] - mult[i] * head
            row = jnp.broadcast_to(x[p][k : k + 1, :], (SUB, TILE))
            for i in below:
                x[i] = x[i] - mult[i] * row
        x[p] = jnp.where(lane <= sub + first, x[p] * root, 0.0)
    return jnp.concatenate(x, axis=0)


def inverse_factor_kernel(gram_ref, out_ref, work, small):
    for tile in range(16):
        for column in range(4):
            row = column * TILE + tile * SUB
            work[row : row + SUB, :] = gram_ref[tile, column]
    out_ref[...] = jnp.zeros_like(out_ref)

    def step(b, carry):
        corner = pl.multiple_of(b * TILE, TILE)
        small[...] = eliminate(work[pl.ds(corner, TILE), pl.ds(corner, TILE)])
        for s in range(RANK // TILE):

            @pl.when(b == s)
            def _():
                at = s * TILE
                end = at + TILE
                inv = small[...]
                out_ref[at:end, at:end] = inv
                if s > 0:
                    done = dot(inv, work[at:end, :at], 1, 0)
                    out_ref[at:end, :at] = done
                if end < RANK:
                    rest = dot(inv, work[at:end, end:], 1, 0)
                    work[end:, end:] -= dot(rest, rest, 0, 0)
                    work[end:, at:end] = -dot(rest, inv, 0, 0)
                    if s > 0:
                        work[end:, :at] -= dot(rest, done, 0, 0)

        return carry

    lax.fori_loop(0, RANK // TILE, step, 0)


def inverse_factor(gram):
    return pl.pallas_call(
        inverse_factor_kernel,
        out_shape=jax.ShapeDtypeStruct((RANK, RANK), jnp.float32),
        in_specs=[pl.BlockSpec(memory_space=pltpu.VMEM)],
        out_specs=pl.BlockSpec(memory_space=pltpu.VMEM),
        scratch_shapes=[
            pltpu.VMEM((RANK, RANK), jnp.float32),
            pltpu.VMEM((TILE, TILE), jnp.float32),
        ],
        cost_estimate=pl.CostEstimate(
            flops=30_000_000_000, bytes_accessed=8 * RANK * RANK, transcendentals=0
        ),
        name="inverse_factor",
    )(gram)


def swap(pieces, axes):
    return lax.all_to_all(pieces, axes, 0, 0, tiled=True)


def to_all(piece, axes):
    devices = lax.axis_size(axes)
    return swap(jnp.broadcast_to(piece[None], (devices, *piece.shape)), axes)


def ring(by, turned=False):
    other = -by if turned else by
    return [(2 * z + c, 2 * ((z + (other if c else by)) % 4) + c) for z in range(4) for c in range(2)]


def neighbours(value, by):
    return lax.ppermute(value, ("zh", "core"), ring(by, turned=True))


def flip(value, axis):
    return lax.ppermute(value, axis, [(0, 1), (1, 0)])


def part(stack, index, dim=0):
    return lax.dynamic_index_in_dim(stack, index, dim, keepdims=False)


def sum_at_owner(rows, axes):
    devices = lax.axis_size(axes)
    return swap(rows.reshape(devices, -1, rows.shape[-1]), axes).sum(axis=0)


def turns(value, axis, by):
    return lax.ppermute(value, axis, [(i, (i + by) % 4) for i in range(4)])


def collect_round(piece, axis, dim=0):
    me = lax.axis_index(axis)
    came = [turns(piece, axis, by) for by in range(1, 4)]
    whole = jnp.stack([piece] * 4, axis=dim)
    for by in range(1, 4):
        whole = lax.dynamic_update_index_in_dim(whole, came[by - 1], (me - by) % 4, dim)
    return whole


def ring_total(value, axis):
    came = [turns(value, axis, by) for by in range(1, 4)]
    return (value + came[1]) + (came[0] + came[2])


def in_pair(value, axis):
    came = flip(value, axis)
    first = lax.axis_index(axis) == 0
    return jnp.concatenate([jnp.where(first, value, came), jnp.where(first, came, value)])


def summed_micro_grad(mine, other, grads):
    even = lax.axis_index("core") == 0

    def product(hidden):
        return lax.dot_general(
            hidden, grads, (((0, 3), (0, 1)), ((), ())), preferred_element_type=jnp.float32
        )

    here = product(mine)
    there = product(other)
    own = jnp.where(even, here[0], there[0])
    across = jnp.where(even, there[0], here[0])

    def code(block):
        top = jnp.maximum(jnp.max(jnp.abs(block), axis=0, keepdims=True), 1e-30)
        power = jnp.ceil(jnp.log2(top)) - 14.0
        coded = (block * jnp.exp2(-power)).astype(jnp.float16)
        return jnp.concatenate([coded, jnp.broadcast_to(power, (16, block.shape[1])).astype(jnp.float16)])

    def sent(coded, by):
        came = neighbours(coded, by).astype(jnp.float32)
        return came[:-16] * jnp.exp2(came[-1:])

    coded = [code(here[1]), code(across), code(there[1])]
    total = own + (sent(coded[0], 1) + sent(coded[1], 2) + sent(coded[2], -1))
    mine, other, *_ = lax.optimization_barrier((mine, other, *coded))
    return total, mine, other


def per_device(momentum, grad_acc, query_basis, hidden_t, out_grad):
    rows, features = momentum.shape
    tokens = hidden_t.shape[1]
    z, core = lax.axis_index("zh"), lax.axis_index("core")
    blocks = hidden_t.reshape(16, 4, rows, tokens)
    wanted = jnp.stack([part(blocks, (z + 2 * core + k) % 4, 1) for k in range(2)], axis=1)
    mine = swap(wanted, PLANE)
    width = features // CHUNKS
    grads = []
    for k in range(CHUNKS):
        piece = out_grad[:, k * width : (k + 1) * width]
        piece = collect_round(piece, PLANE[k])
        piece = collect_round(piece, PLANE[1 - k], 1 - k)
        grads.append(piece.reshape(16, tokens, width))
    other = flip(mine, "core")
    buffers, partial_proj = [], 0.0
    for k in range(CHUNKS):
        at = slice(k * width, (k + 1) * width)
        micro_grad, mine, other = summed_micro_grad(mine, other, grads[k])
        buffers.append(momentum[:, at] + grad_acc[:, at] + micro_grad)
        partial_proj = partial_proj + dot(buffers[-1], query_basis[at], 1, 0, FEWER)
    buffer = jnp.concatenate(buffers, axis=1)

    chip_proj = partial_proj + flip(partial_proj, "core")
    proj = chip_proj + flip(chip_proj, "zl")
    first = lax.axis_index(COLS) * TILE
    strip = dot(lax.dynamic_slice_in_dim(proj, first, TILE, 1), proj, 0, 0)
    strip, proj = lax.optimization_barrier((strip, proj))
    strip = sum_at_owner(strip, PLANE)
    mixed = dot(buffer, proj, 0, 0, FEWER)
    mixed = sum_at_owner(mixed, PLANE)
    strip = ring_total(strip, "zh")
    strip = in_pair(in_pair(strip[None], "core"), "zl")
    gram = to_all(strip.reshape(-1, RANK), PLANE).reshape(16, 4, SUB, RANK)
    mixed = ring_total(mixed, "zh")
    mixed = collect_round(mixed, "y").reshape(-1, RANK)
    mixed = collect_round(mixed, "x").reshape(-1, RANK)

    inv = inverse_factor(gram)
    ortho = dot(proj, inv, 1, 1, FEWER)
    right = dot(mixed, inv, 1, 1, FEWER)
    squares = to_all(jnp.sum(right * right, axis=0)[None], COLS).sum(axis=(0, 1))
    momentum_next = buffer - (1.0 - momentum_keep) * dot(ortho, right, 1, 1, FEWER)
    query_next = right * lax.rsqrt(squares / D + epsilon)
    update = math.sqrt(FF / RANK) * dot(ortho, query_next, 1, 1, FEWER)
    return (update, momentum_next, query_next)


def solution(mesh):
    fine = Mesh(mesh.devices.reshape(4, 4, 4, 2, 2), ROWS + COLS)
    return jax.shard_map(
        per_device,
        mesh=fine,
        in_specs=(
            P(ROWS, COLS),
            P(ROWS, COLS),
            P(COLS, None),
            P(None, ROWS),
            P(ROWS, COLS),
        ),
        out_specs=(P(ROWS, COLS), P(ROWS, COLS), P(COLS, None)),
        check_vma=False,
    )
```

```python
import math

import jax
import jax.numpy as jnp
from jax import lax
from jax.experimental import pallas as pl
from jax.experimental.pallas import tpu as pltpu
from jax.sharding import Mesh
from jax.sharding import PartitionSpec as P


D = 4096
FF = 14336
RANK = 512
TILE = 128
SUB = 8
CHUNKS = 2

momentum_keep = 0.95
epsilon = 1e-06

ROWS = ("x", "y", "zh")
COLS = ("zl", "core")
PLANE = ("x", "y")
FEWER = lax.Precision.HIGH


def dot(left, right, left_dim, right_dim, precision=lax.Precision.HIGHEST):
    return lax.dot_general(
        left,
        right,
        (((left_dim,), (right_dim,)), ((), ())),
        precision=precision,
        preferred_element_type=jnp.float32,
    )


def eliminate(tile):
    lane = lax.broadcasted_iota(jnp.int32, (SUB, TILE), 1)
    sub = lax.broadcasted_iota(jnp.int32, (SUB, TILE), 0)
    x = [tile[SUB * i : SUB * i + SUB, :] for i in range(TILE // SUB)]
    for p in range(TILE // SUB):
        first = SUB * p
        below = range(p, TILE // SUB)
        cols = [
            {i: jnp.broadcast_to(x[i][:, first + k : first + k + 1], (SUB, TILE)) for i in below}
            for k in range(SUB)
        ]
        inside = (lane >= first) & (lane < first + SUB)
        for i in below:
            eye = (lane == sub + first).astype(jnp.float32) if i == p else 0.0
            x[i] = jnp.where(inside, eye, x[i])
        root = jnp.ones((SUB, TILE), jnp.float32)
        for k in range(SUB):
            pivot = jnp.broadcast_to(cols[k][p][k : k + 1, :], (SUB, TILE))
            inverse = 1.0 / pivot
            root = jnp.where(sub == k, lax.rsqrt(pivot), root)
            mult = {i: cols[k][i] * inverse for i in below}
            mult[p] = jnp.where(sub > k, mult[p], 0.0)
            for m in range(k + 1, SUB):
                head = jnp.broadcast_to(cols[m][p][k : k + 1, :], (SUB, TILE))
                for i in below:
                    cols[m][i] = cols[m][i] - mult[i] * head
            row = jnp.broadcast_to(x[p][k : k + 1, :], (SUB, TILE))
            for i in below:
                x[i] = x[i] - mult[i] * row
        x[p] = jnp.where(lane <= sub + first, x[p] * root, 0.0)
    return jnp.concatenate(x, axis=0)


def inverse_factor_kernel(gram_ref, out_ref, work, small):
    for tile in range(16):
        for column in range(4):
            row = column * TILE + tile * SUB
            work[row : row + SUB, :] = gram_ref[tile, column]
    out_ref[...] = jnp.zeros_like(out_ref)

    def step(b, carry):
        corner = pl.multiple_of(b * TILE, TILE)
        small[...] = eliminate(work[pl.ds(corner, TILE), pl.ds(corner, TILE)])
        for s in range(RANK // TILE):

            @pl.when(b == s)
            def _():
                at = s * TILE
                end = at + TILE
                inv = small[...]
                out_ref[at:end, at:end] = inv
                if s > 0:
                    done = dot(inv, work[at:end, :at], 1, 0)
                    out_ref[at:end, :at] = done
                if end < RANK:
                    rest = dot(inv, work[at:end, end:], 1, 0)
                    work[end:, end:] -= dot(rest, rest, 0, 0)
                    work[end:, at:end] = -dot(rest, inv, 0, 0)
                    if s > 0:
                        work[end:, :at] -= dot(rest, done, 0, 0)

        return carry

    lax.fori_loop(0, RANK // TILE, step, 0)


def inverse_factor(gram):
    return pl.pallas_call(
        inverse_factor_kernel,
        out_shape=jax.ShapeDtypeStruct((RANK, RANK), jnp.float32),
        in_specs=[pl.BlockSpec(memory_space=pltpu.VMEM)],
        out_specs=pl.BlockSpec(memory_space=pltpu.VMEM),
        scratch_shapes=[
            pltpu.VMEM((RANK, RANK), jnp.float32),
            pltpu.VMEM((TILE, TILE), jnp.float32),
        ],
        cost_estimate=pl.CostEstimate(
            flops=30_000_000_000, bytes_accessed=8 * RANK * RANK, transcendentals=0
        ),
        name="inverse_factor",
    )(gram)


def swap(pieces, axes):
    return lax.all_to_all(pieces, axes, 0, 0, tiled=True)


def to_all(piece, axes):
    devices = lax.axis_size(axes)
    return swap(jnp.broadcast_to(piece[None], (devices, *piece.shape)), axes)


def ring(by, turned=False):
    other = -by if turned else by
    return [(2 * z + c, 2 * ((z + (other if c else by)) % 4) + c) for z in range(4) for c in range(2)]


def neighbours(value, by):
    return lax.ppermute(value, ("zh", "core"), ring(by, turned=True))


def flip(value, axis):
    return lax.ppermute(value, axis, [(0, 1), (1, 0)])


def part(stack, index, dim=0):
    return lax.dynamic_index_in_dim(stack, index, dim, keepdims=False)


def sum_at_owner(rows, axes):
    devices = lax.axis_size(axes)
    return swap(rows.reshape(devices, -1, rows.shape[-1]), axes).sum(axis=0)


def from_owners(rows, axes):
    return to_all(rows, axes).reshape(-1, rows.shape[-1])


def turns(value, axis, by):
    return lax.ppermute(value, axis, [(i, (i + by) % 4) for i in range(4)])


def collect_round(piece, axis, dim=0):
    me = lax.axis_index(axis)
    came = [turns(piece, axis, by) for by in range(1, 4)]
    whole = jnp.stack([piece] * 4, axis=dim)
    for by in range(1, 4):
        whole = lax.dynamic_update_index_in_dim(whole, came[by - 1], (me - by) % 4, dim)
    return whole


def ring_total(value, axis):
    came = [turns(value, axis, by) for by in range(1, 4)]
    return (value + came[1]) + (came[0] + came[2])


def in_pair(value, axis):
    came = flip(value, axis)
    first = lax.axis_index(axis) == 0
    return jnp.concatenate([jnp.where(first, value, came), jnp.where(first, came, value)])


def summed_micro_grad(mine, other, grads):
    even = lax.axis_index("core") == 0

    def product(hidden):
        return lax.dot_general(
            hidden, grads, (((0, 3), (0, 1)), ((), ())), preferred_element_type=jnp.float32
        )

    here = product(mine)
    there = product(other)
    own = jnp.where(even, here[0], there[0])
    across = jnp.where(even, there[0], here[0])

    def code(block):
        top = jnp.maximum(jnp.max(jnp.abs(block), axis=0, keepdims=True), 1e-30)
        power = jnp.ceil(jnp.log2(top)) - 14.0
        coded = (block * jnp.exp2(-power)).astype(jnp.float16)
        return jnp.concatenate([coded, jnp.broadcast_to(power, (16, block.shape[1])).astype(jnp.float16)])

    def sent(coded, by):
        came = neighbours(coded, by).astype(jnp.float32)
        return came[:-16] * jnp.exp2(came[-1:])

    coded = [code(here[1]), code(across), code(there[1])]
    total = own + (sent(coded[0], 1) + sent(coded[1], 2) + sent(coded[2], -1))
    mine, other, *_ = lax.optimization_barrier((mine, other, *coded))
    return total, mine, other


def per_device(momentum, grad_acc, query_basis, hidden_t, out_grad):
    rows, features = momentum.shape
    tokens = hidden_t.shape[1]
    z, core = lax.axis_index("zh"), lax.axis_index("core")
    blocks = hidden_t.reshape(16, 4, rows, tokens)
    wanted = jnp.stack([part(blocks, (z + 2 * core + k) % 4, 1) for k in range(2)], axis=1)
    mine = swap(wanted, PLANE)
    width = features // CHUNKS
    grads = []
    for k in range(CHUNKS):
        piece = out_grad[:, k * width : (k + 1) * width]
        piece = collect_round(piece, PLANE[k])
        piece = collect_round(piece, PLANE[1 - k], 1 - k)
        grads.append(piece.reshape(16, tokens, width))
    other = flip(mine, "core")
    buffers, partial_proj = [], 0.0
    for k in range(CHUNKS):
        at = slice(k * width, (k + 1) * width)
        micro_grad, mine, other = summed_micro_grad(mine, other, grads[k])
        buffers.append(momentum[:, at] + grad_acc[:, at] + micro_grad)
        partial_proj = partial_proj + dot(buffers[-1], query_basis[at], 1, 0, FEWER)
    buffer = jnp.concatenate(buffers, axis=1)

    chip_proj = partial_proj + flip(partial_proj, "core")
    half = part(chip_proj.reshape(2, -1, RANK), core)
    half = half + flip(half, "zl")
    proj = in_pair(half, "core")
    first = lax.axis_index(COLS) * TILE
    strip = dot(lax.dynamic_slice_in_dim(proj, first, TILE, 1), proj, 0, 0)
    strip, proj = lax.optimization_barrier((strip, proj))
    strip = sum_at_owner(strip, PLANE)
    mixed = dot(buffer, proj, 0, 0, FEWER)
    mixed = sum_at_owner(mixed, PLANE)
    strip = ring_total(strip, "zh")
    strip = in_pair(in_pair(strip[None], "core"), "zl")
    gram = to_all(strip.reshape(-1, RANK), PLANE).reshape(16, 4, SUB, RANK)
    mixed = ring_total(mixed, "zh")
    mixed = from_owners(mixed, PLANE)

    inv = inverse_factor(gram)
    ortho = dot(proj, inv, 1, 1, FEWER)
    right = dot(mixed, inv, 1, 1, FEWER)
    squares = to_all(jnp.sum(right * right, axis=0)[None], COLS).sum(axis=(0, 1))
    momentum_next = buffer - (1.0 - momentum_keep) * dot(ortho, right, 1, 1, FEWER)
    query_next = right * lax.rsqrt(squares / D + epsilon)
    update = math.sqrt(FF / RANK) * dot(ortho, query_next, 1, 1, FEWER)
    return (update, momentum_next, query_next)


def solution(mesh):
    fine = Mesh(mesh.devices.reshape(4, 4, 4, 2, 2), ROWS + COLS)
    return jax.shard_map(
        per_device,
        mesh=fine,
        in_specs=(
            P(ROWS, COLS),
            P(ROWS, COLS),
            P(COLS, None),
            P(None, ROWS),
            P(ROWS, COLS),
        ),
        out_specs=(P(ROWS, COLS), P(ROWS, COLS), P(COLS, None)),
        check_vma=False,
    )
```
